32 devices in a mesh: dp: 2 (over x), col: 4 (over z), row: 4 (over y, core).
Axes of the slice: x: 2, y: 2, z: 4, core: 2. Of those that a mesh axis runs over, the one named last changes fastest.
Arguments:
- left_mat: bfloat16 [65536, 2048], P(('dp', 'row'), 'col'), parts along dimension 0
- right_mat: bfloat16 [2048, 8192], P('row', 'col')
Outputs:
- output: bfloat16 [65536, 8192], P(('dp', 'row'), 'col'), parts along dimension 0
There are 2 independent parts. The reference program is written for one: setup_inputs(seed, part) draws one part's arguments, and reference() takes and returns one part's arrays. A program takes and returns all parts, laid end to end along the dimension named above; an argument that names none is the same for every part.
All inputs are finite; a program needn't handle non-finite values.
Results may differ from the reference program's by a relative error of at most 0.001.
Values are sent between devices in bfloat16 or wider.
A program may use at most 1 GiB of HBM per device.

```python
import jax
import jax.numpy as jnp

ROWS_PART = 32768
D = 2048
FF = 8192


def setup_inputs(seed: int = 0, part: int = 0) -> dict:
    base_key = jax.random.key(seed)
    key_left, key_right = jax.random.split(base_key)
    key_left = jax.random.fold_in(key_left, part)
    left_vals = jax.random.normal(key_left, (ROWS_PART, D), jnp.float32)
    right_vals = jax.random.normal(key_right, (D, FF), jnp.float32) * (D ** -0.5)
    return {"left_mat": left_vals.astype(jnp.bfloat16), "right_mat": right_vals.astype(jnp.bfloat16)}


def reference(left_mat, right_mat):
    full_sum = jnp.dot(left_mat, right_mat, preferred_element_type=jnp.float32)
    return full_sum.astype(jnp.bfloat16)
```

```python
import functools

import jax
import jax.numpy as jnp
from jax import lax
from jax.experimental import pallas as pl
from jax.experimental.pallas import tpu as pltpu
from jax.sharding import PartitionSpec as P


GROUPS = (1536, 1152, 768, 384, 256)
BM = 128


def _mm_kernel(steps, own_p, left_p, opp_p, right_p, own_m, left_m, opp_m, right_m, b_ref, *rest):
    out_ref = rest[-1]
    step = pl.program_id(0)

    def product(own, right, opp, left):
        lhs = jnp.concatenate([own[...], right[...], opp[...], left[...]], axis=1)
        out_ref[...] = jnp.dot(lhs, b_ref[...], preferred_element_type=jnp.float32).astype(out_ref.dtype)

    @pl.when(step < steps)
    def _():
        product(own_p, right_p, opp_p, left_p)

    @pl.when(step >= steps)
    def _():
        product(own_m, right_m, opp_m, left_m)


def _group_product(a, left_p, opp_p, right_p, left_m, opp_m, right_m, b, c, rows, cols, off, size, half):
    bm = min(BM, size)
    steps = size // bm
    depth = a.shape[1]
    total = depth * 4
    first = lambda i: jnp.minimum(i, steps - 1)
    second = lambda i: jnp.maximum(i - steps, 0)
    piece_p = pl.BlockSpec((bm, depth), lambda i: (first(i), 0))
    piece_m = pl.BlockSpec((bm, depth), lambda i: (second(i), 0))
    own_p = pl.BlockSpec((bm, depth), lambda i: (off // bm + first(i), 0))
    own_m = pl.BlockSpec((bm, depth), lambda i: ((half + off) // bm + second(i), 0))
    whole = pl.BlockSpec((total, cols), lambda i: (0, 0), pipeline_mode=pl.Buffered(1))
    out = pl.BlockSpec((bm, cols), lambda i: (jnp.where(i < steps, off // bm + i, (half + off) // bm + i - steps), 0))
    in_specs = [own_p, piece_p, piece_p, piece_p, own_m, piece_m, piece_m, piece_m, whole]
    args = [a, left_p, opp_p, right_p, a, left_m, opp_m, right_m, b]
    alias = {}
    if c is not None:
        in_specs.append(pl.BlockSpec(memory_space=pl.ANY))
        args.append(c)
        alias = {9: 0}
    return pl.pallas_call(
        functools.partial(_mm_kernel, steps),
        grid=(2 * steps,),
        out_shape=jax.ShapeDtypeStruct((rows, cols), jnp.bfloat16),
        in_specs=in_specs,
        out_specs=out,
        input_output_aliases=alias,
        compiler_params=pltpu.CompilerParams(dimension_semantics=("arbitrary",), vmem_limit_bytes=40 * 2**20),
        cost_estimate=pl.CostEstimate(
            flops=2 * 2 * size * total * cols,
            bytes_accessed=2 * size * (total + cols) * 2,
            transcendentals=0,
        ),
        name="group_product",
    )(*args)


def solution(mesh):
    side = mesh.shape["row"]
    up = [(p, (p + 1) % side) for p in range(side)]
    down = [(p, (p - 1) % side) for p in range(side)]

    def local(a, b_own):
        rows, depth = a.shape
        cols = b_own.shape[1]
        half = rows // 2
        offs = [sum(GROUPS[:g]) for g in range(len(GROUPS))]
        row_pos, col_pos = lax.axis_index("row"), lax.axis_index("col")

        a_p = [lax.slice_in_dim(a, o, o + s) for o, s in zip(offs, GROUPS)]
        a_m = [lax.slice_in_dim(a, half + o, half + o + s) for o, s in zip(offs, GROUPS)]
        left_p = [lax.ppermute(x, "col", up) for x in a_p]
        right_m = [lax.ppermute(x, "col", down) for x in a_m]

        b_all = [b_own] + [
            lax.ppermute(b_own, "row", [(p, (p - s) % side) for p in range(side)]) for s in range(1, side)
        ]
        b_twice = jnp.concatenate(b_all + b_all, axis=0)
        b = lax.dynamic_slice_in_dim(b_twice, lax.rem(col_pos - row_pos + side, side) * depth, side * depth)

        c = None
        for g, (off, size) in enumerate(zip(offs, GROUPS)):
            opp_p = lax.ppermute(left_p[g], "col", up)
            opp_m = lax.ppermute(right_m[g], "col", down)
            left_m = lax.ppermute(a_m[g], "col", up)
            right_p = lax.ppermute(a_p[g], "col", down)
            c = _group_product(
                a, left_p[g], opp_p, right_p, left_m, opp_m, right_m[g], b, c, rows, cols, off, size, half
            )
        return c

    return jax.shard_map(
        local, mesh=mesh, in_specs=(P(("dp", "row"), "col"), P("row", "col")),
        out_specs=P(("dp", "row"), "col"), check_vma=False,
    )
```

```python
import functools

import jax
import jax.numpy as jnp
from jax import lax
from jax.experimental import pallas as pl
from jax.experimental.pallas import tpu as pltpu
from jax.sharding import PartitionSpec as P


GROUPS = (1536, 1024, 768, 512, 256)
BM = 256


def _mm_kernel(steps, own_p, left_p, opp_p, right_p, own_m, left_m, opp_m, right_m, b_ref, *rest):
    out_ref = rest[-1]
    step = pl.program_id(0)

    def product(own, right, opp, left):
        lhs = jnp.concatenate([own[...], right[...], opp[...], left[...]], axis=1)
        out_ref[...] = jnp.dot(lhs, b_ref[...], preferred_element_type=jnp.float32).astype(out_ref.dtype)

    @pl.when(step < steps)
    def _():
        product(own_p, right_p, opp_p, left_p)

    @pl.when(step >= steps)
    def _():
        product(own_m, right_m, opp_m, left_m)


def _group_product(a, left_p, opp_p, right_p, left_m, opp_m, right_m, b, c, rows, cols, off, size, half):
    bm = min(BM, size)
    steps = size // bm
    depth = a.shape[1]
    total = depth * 4
    first = lambda i: jnp.minimum(i, steps - 1)
    second = lambda i: jnp.maximum(i - steps, 0)
    piece_p = pl.BlockSpec((bm, depth), lambda i: (first(i), 0))
    piece_m = pl.BlockSpec((bm, depth), lambda i: (second(i), 0))
    own_p = pl.BlockSpec((bm, depth), lambda i: (off // bm + first(i), 0))
    own_m = pl.BlockSpec((bm, depth), lambda i: ((half + off) // bm + second(i), 0))
    whole = pl.BlockSpec((total, cols), lambda i: (0, 0), pipeline_mode=pl.Buffered(1))
    out = pl.BlockSpec((bm, cols), lambda i: (jnp.where(i < steps, off // bm + i, (half + off) // bm + i - steps), 0))
    in_specs = [own_p, piece_p, piece_p, piece_p, own_m, piece_m, piece_m, piece_m, whole]
    args = [a, left_p, opp_p, right_p, a, left_m, opp_m, right_m, b]
    alias = {}
    if c is not None:
        in_specs.append(pl.BlockSpec(memory_space=pl.ANY))
        args.append(c)
        alias = {9: 0}
    return pl.pallas_call(
        functools.partial(_mm_kernel, steps),
        grid=(2 * steps,),
        out_shape=jax.ShapeDtypeStruct((rows, cols), jnp.bfloat16),
        in_specs=in_specs,
        out_specs=out,
        input_output_aliases=alias,
        compiler_params=pltpu.CompilerParams(dimension_semantics=("arbitrary",), vmem_limit_bytes=40 * 2**20),
        cost_estimate=pl.CostEstimate(
            flops=2 * 2 * size * total * cols,
            bytes_accessed=2 * size * (total + cols) * 2,
            transcendentals=0,
        ),
        name="group_product",
    )(*args)


def solution(mesh):
    side = mesh.shape["row"]

    def ring(sense):
        pairs = []
        for col in range(side):
            for row in range(side):
                step = sense if row % 2 == 0 else -sense
                pairs.append((col * side + row, ((col + step) % side) * side + row))
        return pairs

    fwd, bwd = ring(1), ring(-1)
    axes = ("col", "row")

    def local(a, b_own):
        rows, depth = a.shape
        cols = b_own.shape[1]
        half = rows // 2
        offs = [sum(GROUPS[:g]) for g in range(len(GROUPS))]
        row_pos, col_pos = lax.axis_index("row"), lax.axis_index("col")
        sense = 1 - 2 * lax.rem(row_pos, 2)

        a_p = [lax.slice_in_dim(a, o, o + s) for o, s in zip(offs, GROUPS)]
        a_m = [lax.slice_in_dim(a, half + o, half + o + s) for o, s in zip(offs, GROUPS)]
        left_p = [lax.ppermute(x, axes, fwd) for x in a_p]
        right_m = [lax.ppermute(x, axes, bwd) for x in a_m]

        b = jnp.zeros((side * depth, cols), b_own.dtype)
        for s in range(side):
            blk = b_own if s == 0 else lax.ppermute(b_own, "row", [(p, (p - s) % side) for p in range(side)])
            place = lax.rem((row_pos + s - col_pos) * sense + 2 * side, side)
            b = lax.dynamic_update_slice_in_dim(b, blk, place * depth, 0)

        c = None
        for g, (off, size) in enumerate(zip(offs, GROUPS)):
            opp_p = lax.ppermute(left_p[g], axes, fwd)
            opp_m = lax.ppermute(right_m[g], axes, bwd)
            left_m = lax.ppermute(a_m[g], axes, fwd)
            right_p = lax.ppermute(a_p[g], axes, bwd)
            c = _group_product(
                a, left_p[g], opp_p, right_p, left_m, opp_m, right_m[g], b, c, rows, cols, off, size, half
            )
        return c

    return jax.shard_map(
        local, mesh=mesh, in_specs=(P(("dp", "row"), "col"), P("row", "col")),
        out_specs=P(("dp", "row"), "col"), check_vma=False,
    )
```

```python
import jax
import jax.numpy as jnp
from jax import lax
from jax.experimental import pallas as pl
from jax.experimental.pallas import tpu as pltpu
from jax.sharding import PartitionSpec as P


GROUPS = (256, 1024, 1024, 1024, 1024, 1024, 1024, 768, 512, 256, 256)
BM = 256


def _mm_kernel(own, near, far, mid, b_ref, *rest):
    out_ref = rest[-1]
    lhs = jnp.concatenate([own[...], near[...], far[...], mid[...]], axis=1)
    out_ref[...] = jnp.dot(lhs, b_ref[...], preferred_element_type=jnp.float32).astype(out_ref.dtype)


def _group_product(a, near, far, mid, b, c, rows, cols, off, size):
    bm = BM if size > BM else BM // 2
    depth = a.shape[1]
    total = b.shape[0]
    piece = pl.BlockSpec((bm, depth), lambda i: (i, 0))
    own = pl.BlockSpec((bm, depth), lambda i: (off // bm + i, 0))
    whole = pl.BlockSpec((total, cols), lambda i: (0, 0), pipeline_mode=pl.Buffered(1))
    out = pl.BlockSpec((bm, cols), lambda i: (off // bm + i, 0))
    in_specs = [own, piece, piece, piece, whole]
    args = [a, near, far, mid, b]
    alias = {}
    if c is not None:
        in_specs.append(pl.BlockSpec(memory_space=pl.ANY))
        args.append(c)
        alias = {5: 0}
    return pl.pallas_call(
        _mm_kernel,
        grid=(size // bm,),
        out_shape=jax.ShapeDtypeStruct((rows, cols), jnp.bfloat16),
        in_specs=in_specs,
        out_specs=out,
        input_output_aliases=alias,
        compiler_params=pltpu.CompilerParams(dimension_semantics=("arbitrary",), vmem_limit_bytes=28 * 2**20),
        cost_estimate=pl.CostEstimate(
            flops=2 * size * total * cols,
            bytes_accessed=size * (total + cols) * 2,
            transcendentals=0,
        ),
        name="group_product",
    )(*args)


def solution(mesh):
    side = mesh.shape["row"]
    with_near = [(p, p ^ 1) for p in range(side)]
    with_far = [(p, side - 1 - p) for p in range(side)]

    def local(a, b_own):
        rows, depth = a.shape
        cols = b_own.shape[1]
        offs = [sum(GROUPS[:g]) for g in range(len(GROUPS))]
        row_pos, col_pos = lax.axis_index("row"), lax.axis_index("col")

        parts = [lax.slice_in_dim(a, o, o + s) for o, s in zip(offs, GROUPS)]
        near = [lax.ppermute(x, "col", with_near) for x in parts]
        far = [lax.ppermute(x, "col", with_far) for x in parts]
        mid = [lax.ppermute(x, "col", with_near) for x in far]

        b = jnp.zeros((side * depth, cols), b_own.dtype)
        for s in range(side):
            blk = b_own if s == 0 else lax.ppermute(b_own, "row", [(p, (p - s) % side) for p in range(side)])
            rel = lax.rem(row_pos + s, side) ^ col_pos
            b = lax.dynamic_update_slice_in_dim(b, blk, (rel ^ (rel // 2)) * depth, 0)

        c = None
        for g, (off, size) in enumerate(zip(offs, GROUPS)):
            c = _group_product(a, near[g], far[g], mid[g], b, c, rows, cols, off, size)
        return c

    return jax.shard_map(
        local, mesh=mesh, in_specs=(P(("dp", "row"), "col"), P("row", "col")),
        out_specs=P(("dp", "row"), "col"), check_vma=False,
    )
```

```python
import jax
import jax.numpy as jnp
from jax import lax
from jax.experimental import pallas as pl
from jax.experimental.pallas import tpu as pltpu
from jax.sharding import PartitionSpec as P


GROUPS = (256, 1024, 1024, 1024, 1024, 1024, 1024, 768, 512, 256, 128, 128)
BM = 256


def _mm_kernel(own, near, far, mid, b_ref, *rest):
    out_ref = rest[-1]
    lhs = jnp.concatenate([own[...], near[...], far[...], mid[...]], axis=1)
    out_ref[...] = jnp.dot(lhs, b_ref[...], preferred_element_type=jnp.float32).astype(out_ref.dtype)


def _group_product(own, near, far, mid, b, c, rows, cols, off, size):
    bm = BM if size > BM else BM // 2
    depth = own.shape[1]
    total = b.shape[0]
    piece = pl.BlockSpec((bm, depth), lambda i: (i, 0))
    whole = pl.BlockSpec((total, cols), lambda i: (0, 0), pipeline_mode=pl.Buffered(1))
    out = pl.BlockSpec((bm, cols), lambda i: (off // bm + i, 0))
    in_specs = [piece, piece, piece, piece, whole]
    args = [own, near, far, mid, b]
    alias = {}
    if c is not None:
        in_specs.append(pl.BlockSpec(memory_space=pl.ANY))
        args.append(c)
        alias = {5: 0}
    return pl.pallas_call(
        _mm_kernel,
        grid=(size // bm,),
        out_shape=jax.ShapeDtypeStruct((rows, cols), jnp.bfloat16),
        in_specs=in_specs,
        out_specs=out,
        input_output_aliases=alias,
        compiler_params=pltpu.CompilerParams(dimension_semantics=("arbitrary",), vmem_limit_bytes=20 * 2**20),
        cost_estimate=pl.CostEstimate(
            flops=2 * size * total * cols,
            bytes_accessed=size * (total + cols) * 2,
            transcendentals=0,
        ),
        name="group_product",
    )(*args)


def _stack_kernel(place_ref, *refs):
    sems = refs[-1]
    out_ref = refs[-2]
    depth = refs[0].shape[0]
    copies = [
        pltpu.make_async_copy(ref, out_ref.at[pl.ds(pl.multiple_of(place_ref[s] * depth, depth), depth)], sems.at[s])
        for s, ref in enumerate(refs[:-2])
    ]
    for copy in copies:
        copy.start()
    for copy in copies:
        copy.wait()


def _stack_blocks(places, blocks):
    count = len(blocks)
    depth, cols = blocks[0].shape
    return pl.pallas_call(
        _stack_kernel,
        out_shape=pltpu.VMEM((count * depth, cols), blocks[0].dtype),
        in_specs=[pl.BlockSpec(memory_space=pltpu.SMEM)] + [pl.BlockSpec(memory_space=pl.ANY)] * count,
        out_specs=pl.BlockSpec(memory_space=pltpu.VMEM),
        scratch_shapes=[pltpu.SemaphoreType.DMA((count,))],
        cost_estimate=pl.CostEstimate(flops=2**20, bytes_accessed=2 * count * depth * cols * 2, transcendentals=0),
        compiler_params=pltpu.CompilerParams(vmem_limit_bytes=12 * 2**20),
        name="stack_blocks",
    )(places, *blocks)


def solution(mesh):
    side = mesh.shape["row"]
    with_near = [(p, p ^ 1) for p in range(side)]
    with_far = [(p, side - 1 - p) for p in range(side)]

    def local(a, b_own):
        rows, _ = a.shape
        cols = b_own.shape[1]
        offs = [sum(GROUPS[:g]) for g in range(len(GROUPS))]
        row_pos, col_pos = lax.axis_index("row"), lax.axis_index("col")

        parts = [lax.slice_in_dim(a, o, o + s) for o, s in zip(offs, GROUPS)]
        near = [lax.ppermute(x, "col", with_near) for x in parts]
        far = [lax.ppermute(x, "col", with_far) for x in parts]
        mid = [lax.ppermute(x, "col", with_near) for x in far]

        blocks = [b_own] + [
            lax.ppermute(b_own, "row", [(p, (p - s) % side) for p in range(side)]) for s in range(1, side)
        ]
        rels = [lax.rem(row_pos + s, side) ^ col_pos for s in range(side)]
        b = _stack_blocks(jnp.stack([rel ^ (rel // 2) for rel in rels]), blocks)

        c = None
        for g, (off, size) in enumerate(zip(offs, GROUPS)):
            c = _group_product(parts[g], near[g], far[g], mid[g], b, c, rows, cols, off, size)
        return c

    return jax.shard_map(
        local, mesh=mesh, in_specs=(P(("dp", "row"), "col"), P("row", "col")),
        out_specs=P(("dp", "row"), "col"), check_vma=False,
    )
```

```python
import functools

import jax
import jax.numpy as jnp
from jax import lax
from jax.experimental import pallas as pl
from jax.experimental.pallas import tpu as pltpu
from jax.sharding import PartitionSpec as P


HALVES = 4
GROUPS = (1024, 1024, 1024, 1024, 1024, 1024, 1024, 512, 256, 128, 128)
BM = 256


def _mm_kernel(side, own, near, p2, p3, p4, p5, b_ref, *rest):
    out_ref = rest[-1]
    col_pos = lax.axis_index("col")
    at_end = jnp.logical_or(col_pos == 0, col_pos == side - 1)

    third = jnp.where(at_end, p3[...], p4[...])
    fourth = jnp.where(at_end, p5[...], p2[...])
    lhs = jnp.concatenate([own[...], near[...], third, fourth], axis=1)
    out_ref[...] = jnp.dot(lhs, b_ref[...], preferred_element_type=jnp.float32).astype(out_ref.dtype)


def _group_product(side, a, near, p2, p3, p4, p5, b, c, off, size):
    bm = BM if size > BM else BM // 2
    rows, depth = a.shape
    total, cols = b.shape
    base = off % p2.shape[0]
    piece = pl.BlockSpec((bm, depth), lambda i: (i, 0))
    chunk = pl.BlockSpec((bm, depth), lambda i: (base // bm + i, 0))
    full = pl.BlockSpec((bm, depth), lambda i: (off // bm + i, 0))
    whole = pl.BlockSpec((total, cols), lambda i: (0, 0), pipeline_mode=pl.Buffered(1))
    out = pl.BlockSpec((bm, cols), lambda i: (off // bm + i, 0))
    in_specs = [full, full, chunk, chunk, piece, piece, whole]
    args = [a, near, p2, p3, p4, p5, b]
    alias = {}
    if c is not None:
        in_specs.append(pl.BlockSpec(memory_space=pl.ANY))
        args.append(c)
        alias = {7: 0}
    return pl.pallas_call(
        functools.partial(_mm_kernel, side),
        grid=(size // bm,),
        out_shape=jax.ShapeDtypeStruct((rows, cols), jnp.bfloat16),
        in_specs=in_specs,
        out_specs=out,
        input_output_aliases=alias,
        compiler_params=pltpu.CompilerParams(dimension_semantics=("arbitrary",), vmem_limit_bytes=22 * 2**20),
        cost_estimate=pl.CostEstimate(
            flops=2 * size * total * cols,
            bytes_accessed=size * (total + cols) * 2,
            transcendentals=0,
        ),
        name="group_product",
    )(*args)


def _stack_kernel(place_ref, *refs):
    sems = refs[-1]
    out_ref = refs[-2]
    depth = refs[0].shape[0]
    copies = [
        pltpu.make_async_copy(ref, out_ref.at[pl.ds(pl.multiple_of(place_ref[s] * depth, depth), depth)], sems.at[s])
        for s, ref in enumerate(refs[:-2])
    ]
    for copy in copies:
        copy.start()
    for copy in copies:
        copy.wait()


def _stack_blocks(places, blocks):
    count = len(blocks)
    depth, cols = blocks[0].shape
    return pl.pallas_call(
        _stack_kernel,
        out_shape=pltpu.VMEM((count * depth, cols), blocks[0].dtype),
        in_specs=[pl.BlockSpec(memory_space=pltpu.SMEM)] + [pl.BlockSpec(memory_space=pl.ANY)] * count,
        out_specs=pl.BlockSpec(memory_space=pltpu.VMEM),
        scratch_shapes=[pltpu.SemaphoreType.DMA((count,))],
        cost_estimate=pl.CostEstimate(flops=2**20, bytes_accessed=2 * count * depth * cols * 2, transcendentals=0),
        compiler_params=pltpu.CompilerParams(vmem_limit_bytes=12 * 2**20),
        name="stack_blocks",
    )(places, *blocks)


def solution(mesh):
    side = mesh.shape["row"]
    with_near = [(p, p ^ 1) for p in range(side)]
    inner = [(p, side - 1 - p if 0 < p < side - 1 else p) for p in range(side)]

    def local(a, b_own):
        rows, _ = a.shape
        offs = [sum(GROUPS[:g]) for g in range(len(GROUPS))]
        row_pos, col_pos = lax.axis_index("row"), lax.axis_index("col")

        near = lax.ppermute(a, "col", with_near)
        step = rows // HALVES
        p2 = [lax.ppermute(a[h * step : (h + 1) * step], "col", inner) for h in range(HALVES)]
        p3 = [lax.ppermute(x, "col", with_near) for x in p2]
        p4 = [lax.ppermute(near[o : o + s], "col", inner) for o, s in zip(offs, GROUPS)]
        p5 = [lax.ppermute(x, "col", with_near) for x in p4]

        blocks = [b_own] + [
            lax.ppermute(b_own, "row", [(p, (p - s) % side) for p in range(side)]) for s in range(1, side)
        ]
        b = _stack_blocks(jnp.stack([lax.rem(row_pos + s, side) ^ col_pos for s in range(side)]), blocks)

        c = None
        for g, (off, size) in enumerate(zip(offs, GROUPS)):
            h = off // step
            c = _group_product(side, a, near, p2[h], p3[h], p4[g], p5[g], b, c, off, size)
        return c

    return jax.shard_map(
        local, mesh=mesh, in_specs=(P(("dp", "row"), "col"), P("row", "col")),
        out_specs=P(("dp", "row"), "col"), check_vma=False,
    )
```

```python
import functools

import jax
import jax.numpy as jnp
from jax import lax
from jax.experimental import pallas as pl
from jax.experimental.pallas import tpu as pltpu
from jax.sharding import PartitionSpec as P


HALVES = 4
GROUPS = (1024, 1024, 1024, 1024, 1024, 1024, 1024)
TAIL = (512, 256, 128, 128)
BM = 256


def _at_end(side):
    col_pos = lax.axis_index("col")
    return jnp.logical_or(col_pos == 0, col_pos == side - 1)


def _mm_kernel(side, own, near, p2, p3, p4, p5, b_ref, *rest):
    out_ref = rest[-1]
    at_end = _at_end(side)
    third = jnp.where(at_end, p3[...], p4[...])
    fourth = jnp.where(at_end, p5[...], p2[...])
    lhs = jnp.concatenate([own[...], near[...], third, fourth], axis=1)
    out_ref[...] = jnp.dot(lhs, b_ref[...], preferred_element_type=jnp.float32).astype(out_ref.dtype)


def _early_kernel(side, own, near, p3, p4, b_ref, out_ref):
    third = jnp.where(_at_end(side), p3[...], p4[...])
    lhs = jnp.concatenate([own[...], near[...], third], axis=1)
    out_ref[...] = jnp.dot(lhs, b_ref[: lhs.shape[1], :], preferred_element_type=jnp.float32)


def _late_kernel(side, p2, p5, b_ref, early, c_in, out_ref):
    fourth = jnp.where(_at_end(side), p5[...], p2[...])
    depth = fourth.shape[1]
    total = early[...] + jnp.dot(fourth, b_ref[-depth:, :], preferred_element_type=jnp.float32)
    out_ref[...] = total.astype(out_ref.dtype)


def _rows(bm, depth, off):
    return pl.BlockSpec((bm, depth), lambda i: (off // bm + i, 0))


def _kept(shape):
    return pl.BlockSpec(shape, lambda i: (0, 0), pipeline_mode=pl.Buffered(1))


def _params(vmem_mib):
    return pltpu.CompilerParams(dimension_semantics=("arbitrary",), vmem_limit_bytes=vmem_mib * 2**20)


def _cost(size, depth, cols):
    return pl.CostEstimate(
        flops=2 * size * depth * cols, bytes_accessed=2 * size * (depth + cols), transcendentals=0
    )


def _group_product(side, a, near, p2, p3, p4, p5, b, c, off, size):
    rows, depth = a.shape
    total, cols = b.shape
    full = _rows(BM, depth, off)
    chunk = _rows(BM, depth, off % p2.shape[0])
    piece = _rows(BM, depth, 0)
    in_specs = [full, full, chunk, chunk, piece, piece, _kept(b.shape)]
    args = [a, near, p2, p3, p4, p5, b]
    alias = {}
    if c is not None:
        in_specs.append(pl.BlockSpec(memory_space=pl.ANY))
        args.append(c)
        alias = {7: 0}
    return pl.pallas_call(
        functools.partial(_mm_kernel, side),
        grid=(size // BM,),
        out_shape=jax.ShapeDtypeStruct((rows, cols), jnp.bfloat16),
        in_specs=in_specs,
        out_specs=_rows(BM, cols, off),
        input_output_aliases=alias,
        compiler_params=_params(16),
        cost_estimate=_cost(size, total, cols),
        name="group_product",
    )(*args)


def _early_product(side, a, near, p3, p4, b, off, size):
    depth = a.shape[1]
    cols = b.shape[1]
    bm = min(BM, size)
    full = _rows(bm, depth, off)
    return pl.pallas_call(
        functools.partial(_early_kernel, side),
        grid=(size // bm,),
        out_shape=pltpu.VMEM((size, cols), jnp.float32),
        in_specs=[full, full, _rows(bm, depth, off % p3.shape[0]), _rows(bm, depth, 0), _kept(b.shape)],
        out_specs=_rows(bm, cols, 0),
        compiler_params=_params(20),
        cost_estimate=_cost(size, 3 * depth, cols),
        name="early_product",
    )(a, near, p3, p4, b)


def _late_product(side, p2, p5, b, early, c, off, size):
    depth = p5.shape[1]
    rows, cols = c.shape
    bm = BM // 2
    return pl.pallas_call(
        functools.partial(_late_kernel, side),
        grid=(size // bm,),
        out_shape=jax.ShapeDtypeStruct((rows, cols), jnp.bfloat16),
        in_specs=[
            _rows(bm, depth, off % p2.shape[0]), _rows(bm, depth, 0), _kept(b.shape), _rows(bm, cols, 0),
            pl.BlockSpec(memory_space=pl.ANY),
        ],
        out_specs=_rows(bm, cols, off),
        input_output_aliases={4: 0},
        compiler_params=_params(16),
        cost_estimate=_cost(size, depth, cols),
        name="late_product",
    )(p2, p5, b, early, c)


def _stack_kernel(place_ref, *refs):
    sems = refs[-1]
    out_ref = refs[-2]
    depth = refs[0].shape[0]
    copies = [
        pltpu.make_async_copy(ref, out_ref.at[pl.ds(pl.multiple_of(place_ref[s] * depth, depth), depth)], sems.at[s])
        for s, ref in enumerate(refs[:-2])
    ]
    for copy in copies:
        copy.start()
    for copy in copies:
        copy.wait()


def _stack_blocks(places, blocks):
    count = len(blocks)
    depth, cols = blocks[0].shape
    return pl.pallas_call(
        _stack_kernel,
        out_shape=pltpu.VMEM((count * depth, cols), blocks[0].dtype),
        in_specs=[pl.BlockSpec(memory_space=pltpu.SMEM)] + [pl.BlockSpec(memory_space=pl.ANY)] * count,
        out_specs=pl.BlockSpec(memory_space=pltpu.VMEM),
        scratch_shapes=[pltpu.SemaphoreType.DMA((count,))],
        cost_estimate=pl.CostEstimate(flops=2**20, bytes_accessed=2 * count * depth * cols * 2, transcendentals=0),
        compiler_params=pltpu.CompilerParams(vmem_limit_bytes=12 * 2**20),
        name="stack_blocks",
    )(places, *blocks)


def solution(mesh):
    side = mesh.shape["row"]
    with_near = [(p, p ^ 1) for p in range(side)]
    inner = [(p, side - 1 - p if 0 < p < side - 1 else p) for p in range(side)]

    def local(a, b_own):
        rows, _ = a.shape
        sizes = GROUPS + TAIL
        offs = [sum(sizes[:g]) for g in range(len(sizes))]
        row_pos, col_pos = lax.axis_index("row"), lax.axis_index("col")

        near = lax.ppermute(a, "col", with_near)
        step = rows // HALVES
        p2 = [lax.ppermute(a[h * step : (h + 1) * step], "col", inner) for h in range(HALVES)]
        p3 = [lax.ppermute(x, "col", with_near) for x in p2]
        p4 = [lax.ppermute(near[o : o + s], "col", inner) for o, s in zip(offs, sizes)]
        p5 = [lax.ppermute(x, "col", with_near) for x in p4]

        blocks = [b_own] + [
            lax.ppermute(b_own, "row", [(p, (p - s) % side) for p in range(side)]) for s in range(1, side)
        ]
        b = _stack_blocks(jnp.stack([lax.rem(row_pos + s, side) ^ col_pos for s in range(side)]), blocks)

        main = len(GROUPS)
        early = []
        for g in range(main, len(sizes)):
            early.append(_early_product(side, a, near, p3[offs[g] // step], p4[g], b, offs[g], sizes[g]))

        c = None
        for g, (off, size) in enumerate(zip(offs, sizes)):
            h = off // step
            if g < main:
                c = _group_product(side, a, near, p2[h], p3[h], p4[g], p5[g], b, c, off, size)
            else:
                c = _late_product(side, p2[h], p5[g], b, early[g - main], c, off, size)
        return c

    return jax.shard_map(
        local, mesh=mesh, in_specs=(P(("dp", "row"), "col"), P("row", "col")),
        out_specs=P(("dp", "row"), "col"), check_vma=False,
    )
```

```python
import functools

import jax
import jax.numpy as jnp
from jax import lax
from jax.experimental import pallas as pl
from jax.experimental.pallas import tpu as pltpu
from jax.sharding import PartitionSpec as P


HALVES = 4
GROUPS = (1024, 1024, 1024, 1024, 1024, 1024, 1024)
TAIL = (512, 256, 128, 128)
BM = 256
LATE_STEPS = 1


def _at_end(side):
    col_pos = lax.axis_index("col")
    return jnp.logical_or(col_pos == 0, col_pos == side - 1)


def _mm_kernel(side, own, near, p2, p3, p4, p5, b_ref, *rest):
    out_ref = rest[-1]
    at_end = _at_end(side)
    third = jnp.where(at_end, p3[...], p4[...])
    fourth = jnp.where(at_end, p5[...], p2[...])
    lhs = jnp.concatenate([own[...], near[...], third, fourth], axis=1)
    out_ref[...] = jnp.dot(lhs, b_ref[...], preferred_element_type=jnp.float32).astype(out_ref.dtype)


def _early_kernel(side, own, near, p2, p3, p4, b_ref, out_ref):
    at_end = _at_end(side)
    third = jnp.where(at_end, p3[...], p4[...])
    fourth = jnp.where(at_end, jnp.zeros_like(p2), p2[...])
    lhs = jnp.concatenate([own[...], near[...], third, fourth], axis=1)
    out_ref[...] = jnp.dot(lhs, b_ref[...], preferred_element_type=jnp.float32)


def _late_kernel(side, p5, b_ref, early, c_in, out_ref):
    depth = p5.shape[1]
    fourth = jnp.where(_at_end(side), p5[...], jnp.zeros_like(p5))
    total = early[...] + jnp.dot(fourth, b_ref[-depth:, :], preferred_element_type=jnp.float32)
    out_ref[...] = total.astype(out_ref.dtype)


def _rows(bm, depth, off):
    return pl.BlockSpec((bm, depth), lambda i: (off // bm + i, 0))


def _kept(shape):
    return pl.BlockSpec(shape, lambda i: (0, 0), pipeline_mode=pl.Buffered(1))


def _params(vmem_mib):
    return pltpu.CompilerParams(dimension_semantics=("arbitrary",), vmem_limit_bytes=vmem_mib * 2**20)


def _cost(size, depth, cols):
    return pl.CostEstimate(
        flops=2 * size * depth * cols, bytes_accessed=2 * size * (depth + cols), transcendentals=0
    )


def _group_product(side, own, near, p2, p3, p4, p5, b, c, rows, off, size):
    depth = own.shape[1]
    total, cols = b.shape
    chunk = _rows(BM, depth, off % p2.shape[0])
    piece = _rows(BM, depth, 0)
    in_specs = [chunk, piece, chunk, chunk, piece, piece, _kept(b.shape)]
    args = [own, near, p2, p3, p4, p5, b]
    alias = {}
    if c is not None:
        in_specs.append(pl.BlockSpec(memory_space=pl.ANY))
        args.append(c)
        alias = {7: 0}
    return pl.pallas_call(
        functools.partial(_mm_kernel, side),
        grid=(size // BM,),
        out_shape=jax.ShapeDtypeStruct((rows, cols), jnp.bfloat16),
        in_specs=in_specs,
        out_specs=_rows(BM, cols, off),
        input_output_aliases=alias,
        compiler_params=_params(8),
        cost_estimate=_cost(size, total, cols),
        name="group_product",
    )(*args)


def _early_product(side, own, near, p2, p3, p4, b, off, size):
    depth = own.shape[1]
    total, cols = b.shape
    bm = min(BM, size)
    chunk = _rows(bm, depth, off % p3.shape[0])
    piece = _rows(bm, depth, 0)
    return pl.pallas_call(
        functools.partial(_early_kernel, side),
        grid=(size // bm,),
        out_shape=pltpu.VMEM((size, cols), jnp.float32),
        in_specs=[chunk, piece, chunk, chunk, piece, _kept(b.shape)],
        out_specs=_rows(bm, cols, 0),
        compiler_params=_params(8),
        cost_estimate=_cost(size, total, cols),
        name="early_product",
    )(own, near, p2, p3, p4, b)


def _late_product(side, p5, b, early, c, off, size):
    depth = p5.shape[1]
    rows, cols = c.shape
    bm = min(BM, size) // LATE_STEPS
    return pl.pallas_call(
        functools.partial(_late_kernel, side),
        grid=(size // bm,),
        out_shape=jax.ShapeDtypeStruct((rows, cols), jnp.bfloat16),
        in_specs=[
            _rows(bm, depth, 0), _kept(b.shape), _rows(bm, cols, 0), pl.BlockSpec(memory_space=pl.ANY),
        ],
        out_specs=_rows(bm, cols, off),
        input_output_aliases={3: 0},
        compiler_params=_params(8),
        cost_estimate=_cost(size, depth, cols),
        name="late_product",
    )(p5, b, early, c)


def _stack_kernel(place_ref, *refs):
    sems = refs[-1]
    out_ref = refs[-2]
    depth = refs[0].shape[0]
    copies = [
        pltpu.make_async_copy(ref, out_ref.at[pl.ds(pl.multiple_of(place_ref[s] * depth, depth), depth)], sems.at[s])
        for s, ref in enumerate(refs[:-2])
    ]
    for copy in copies:
        copy.start()
    for copy in copies:
        copy.wait()


def _stack_blocks(places, blocks):
    count = len(blocks)
    depth, cols = blocks[0].shape
    return pl.pallas_call(
        _stack_kernel,
        out_shape=pltpu.VMEM((count * depth, cols), blocks[0].dtype),
        in_specs=[pl.BlockSpec(memory_space=pltpu.SMEM)] + [pl.BlockSpec(memory_space=pl.ANY)] * count,
        out_specs=pl.BlockSpec(memory_space=pltpu.VMEM),
        scratch_shapes=[pltpu.SemaphoreType.DMA((count,))],
        cost_estimate=pl.CostEstimate(flops=2**20, bytes_accessed=2 * count * depth * cols * 2, transcendentals=0),
        compiler_params=pltpu.CompilerParams(vmem_limit_bytes=12 * 2**20),
        name="stack_blocks",
    )(places, *blocks)


def solution(mesh):
    side = mesh.shape["row"]
    with_near = [(p, p ^ 1) for p in range(side)]
    inner = [(p, side - 1 - p if 0 < p < side - 1 else p) for p in range(side)]

    def local(a, b_own):
        rows, _ = a.shape
        sizes = GROUPS + TAIL
        offs = [sum(sizes[:g]) for g in range(len(sizes))]
        row_pos, col_pos = lax.axis_index("row"), lax.axis_index("col")

        near = lax.ppermute(a, "col", with_near)
        step = rows // HALVES
        own = [a[h * step : (h + 1) * step] for h in range(HALVES)]
        p2 = [lax.ppermute(x, "col", inner) for x in own]
        p3 = [lax.ppermute(x, "col", with_near) for x in p2]
        near = [near[o : o + s] for o, s in zip(offs, sizes)]
        p4 = [lax.ppermute(x, "col", inner) for x in near]
        p5 = [lax.ppermute(x, "col", with_near) for x in p4]

        blocks = [b_own] + [
            lax.ppermute(b_own, "row", [(p, (p - s) % side) for p in range(side)]) for s in range(1, side)
        ]
        b = _stack_blocks(jnp.stack([lax.rem(row_pos + s, side) ^ col_pos for s in range(side)]), blocks)

        main = len(GROUPS)
        early = {}
        for g in range(main, len(sizes)):
            h = offs[g] // step
            early[g] = _early_product(side, own[h], near[g], p2[h], p3[h], p4[g], b, offs[g], sizes[g])

        c = None
        for g, (off, size) in enumerate(zip(offs, sizes)):
            h = off // step
            if g < main:
                c = _group_product(side, own[h], near[g], p2[h], p3[h], p4[g], p5[g], b, c, rows, off, size)
            else:
                c = _late_product(side, p5[g], b, early[g], c, off, size)
        return c

    return jax.shard_map(
        local, mesh=mesh, in_specs=(P(("dp", "row"), "col"), P("row", "col")),
        out_specs=P(("dp", "row"), "col"), check_vma=False,
    )
```

```python
import functools

import jax
import jax.numpy as jnp
from jax import lax
from jax.experimental import pallas as pl
from jax.experimental.pallas import tpu as pltpu
from jax.sharding import PartitionSpec as P


HALVES = 4
GROUPS = (2048, 2048, 2048, 1024)
TAIL = (512, 256, 128, 128)
BM = 256
LATE_STEPS = 1


def _at_end(side):
    col_pos = lax.axis_index("col")
    return jnp.logical_or(col_pos == 0, col_pos == side - 1)


def _mm_kernel(side, own, near, p2, p3, p4, p5, b_ref, *rest):
    out_ref = rest[-1]
    at_end = _at_end(side)
    third = jnp.where(at_end, p3[...], p4[...])
    fourth = jnp.where(at_end, p5[...], p2[...])
    lhs = jnp.concatenate([own[...], near[...], third, fourth], axis=1)
    out_ref[...] = jnp.dot(lhs, b_ref[...], preferred_element_type=jnp.float32).astype(out_ref.dtype)


def _early_kernel(side, own, near, p2, p3, p4, b_ref, out_ref):
    at_end = _at_end(side)
    third = jnp.where(at_end, p3[...], p4[...])
    fourth = jnp.where(at_end, jnp.zeros_like(p2), p2[...])
    lhs = jnp.concatenate([own[...], near[...], third, fourth], axis=1)
    out_ref[...] = jnp.dot(lhs, b_ref[...], preferred_element_type=jnp.float32)


def _late_kernel(side, p5, b_ref, early, c_in, out_ref):
    depth = p5.shape[1]
    fourth = jnp.where(_at_end(side), p5[...], jnp.zeros_like(p5))
    total = early[...] + jnp.dot(fourth, b_ref[-depth:, :], preferred_element_type=jnp.float32)
    out_ref[...] = total.astype(out_ref.dtype)


def _rows(bm, depth, off):
    return pl.BlockSpec((bm, depth), lambda i: (off // bm + i, 0))


def _kept(shape):
    return pl.BlockSpec(shape, lambda i: (0, 0), pipeline_mode=pl.Buffered(1))


def _params(vmem_mib):
    return pltpu.CompilerParams(dimension_semantics=("arbitrary",), vmem_limit_bytes=vmem_mib * 2**20)


def _cost(size, depth, cols):
    return pl.CostEstimate(
        flops=2 * size * depth * cols, bytes_accessed=2 * size * (depth + cols), transcendentals=0
    )


def _group_product(side, own, near, p2, p3, p4, p5, b, c, rows, off, size):
    depth = own.shape[1]
    total, cols = b.shape
    chunk = _rows(BM, depth, off % p2.shape[0])
    piece = _rows(BM, depth, 0)
    full = _rows(BM, depth, off)
    in_specs = [full, full, chunk, chunk, piece, piece, _kept(b.shape)]
    args = [own, near, p2, p3, p4, p5, b]
    alias = {}
    if c is not None:
        in_specs.append(pl.BlockSpec(memory_space=pl.ANY))
        args.append(c)
        alias = {7: 0}
    return pl.pallas_call(
        functools.partial(_mm_kernel, side),
        grid=(size // BM,),
        out_shape=jax.ShapeDtypeStruct((rows, cols), jnp.bfloat16),
        in_specs=in_specs,
        out_specs=_rows(BM, cols, off),
        input_output_aliases=alias,
        compiler_params=_params(8),
        cost_estimate=_cost(size, total, cols),
        name="group_product",
    )(*args)


def _early_product(side, own, near, p2, p3, p4, b, off, size):
    depth = own.shape[1]
    total, cols = b.shape
    bm = min(BM, size)
    full = _rows(bm, depth, off)
    chunk = _rows(bm, depth, off % p3.shape[0])
    piece = _rows(bm, depth, 0)
    return pl.pallas_call(
        functools.partial(_early_kernel, side),
        grid=(size // bm,),
        out_shape=pltpu.VMEM((size, cols), jnp.float32),
        in_specs=[full, full, chunk, chunk, piece, _kept(b.shape)],
        out_specs=_rows(bm, cols, 0),
        compiler_params=_params(8),
        cost_estimate=_cost(size, total, cols),
        name="early_product",
    )(own, near, p2, p3, p4, b)


def _late_product(side, p5, b, early, c, off, size):
    depth = p5.shape[1]
    rows, cols = c.shape
    bm = min(BM, size) // LATE_STEPS
    return pl.pallas_call(
        functools.partial(_late_kernel, side),
        grid=(size // bm,),
        out_shape=jax.ShapeDtypeStruct((rows, cols), jnp.bfloat16),
        in_specs=[
            _rows(bm, depth, 0), _kept(b.shape), _rows(bm, cols, 0), pl.BlockSpec(memory_space=pl.ANY),
        ],
        out_specs=_rows(bm, cols, off),
        input_output_aliases={3: 0},
        compiler_params=_params(8),
        cost_estimate=_cost(size, depth, cols),
        name="late_product",
    )(p5, b, early, c)


def _stack_kernel(place_ref, *refs):
    sems = refs[-1]
    out_ref = refs[-2]
    depth = refs[0].shape[0]
    copies = [
        pltpu.make_async_copy(ref, out_ref.at[pl.ds(pl.multiple_of(place_ref[s] * depth, depth), depth)], sems.at[s])
        for s, ref in enumerate(refs[:-2])
    ]
    for copy in copies:
        copy.start()
    for copy in copies:
        copy.wait()


def _stack_blocks(places, blocks):
    count = len(blocks)
    depth, cols = blocks[0].shape
    return pl.pallas_call(
        _stack_kernel,
        out_shape=pltpu.VMEM((count * depth, cols), blocks[0].dtype),
        in_specs=[pl.BlockSpec(memory_space=pltpu.SMEM)] + [pl.BlockSpec(memory_space=pl.ANY)] * count,
        out_specs=pl.BlockSpec(memory_space=pltpu.VMEM),
        scratch_shapes=[pltpu.SemaphoreType.DMA((count,))],
        cost_estimate=pl.CostEstimate(flops=2**20, bytes_accessed=2 * count * depth * cols * 2, transcendentals=0),
        compiler_params=pltpu.CompilerParams(vmem_limit_bytes=12 * 2**20),
        name="stack_blocks",
    )(places, *blocks)


def solution(mesh):
    side = mesh.shape["row"]
    with_near = [(p, p ^ 1) for p in range(side)]
    inner = [(p, side - 1 - p if 0 < p < side - 1 else p) for p in range(side)]

    def local(a, b_own):
        rows, _ = a.shape
        sizes = GROUPS + TAIL
        offs = [sum(sizes[:g]) for g in range(len(sizes))]
        row_pos, col_pos = lax.axis_index("row"), lax.axis_index("col")

        near = lax.ppermute(a, "col", with_near)
        step = rows // HALVES
        p2 = [lax.ppermute(a[h * step : (h + 1) * step], "col", inner) for h in range(HALVES)]
        p3 = [lax.ppermute(x, "col", with_near) for x in p2]
        p4 = [lax.ppermute(near[o : o + s], "col", inner) for o, s in zip(offs, sizes)]
        p5 = [lax.ppermute(x, "col", with_near) for x in p4]

        blocks = [b_own] + [
            lax.ppermute(b_own, "row", [(p, (p - s) % side) for p in range(side)]) for s in range(1, side)
        ]
        b = _stack_blocks(jnp.stack([lax.rem(row_pos + s, side) ^ col_pos for s in range(side)]), blocks)

        main = len(GROUPS)
        early = {}
        for g in range(main, len(sizes)):
            h = offs[g] // step
            early[g] = _early_product(side, a, near, p2[h], p3[h], p4[g], b, offs[g], sizes[g])

        c = None
        for g, (off, size) in enumerate(zip(offs, sizes)):
            h = off // step
            if g < main:
                c = _group_product(side, a, near, p2[h], p3[h], p4[g], p5[g], b, c, rows, off, size)
            else:
                c = _late_product(side, p5[g], b, early[g], c, off, size)
        return c

    return jax.shard_map(
        local, mesh=mesh, in_specs=(P(("dp", "row"), "col"), P("row", "col")),
        out_specs=P(("dp", "row"), "col"), check_vma=False,
    )
```

```python
import functools

import jax
import jax.numpy as jnp
from jax import lax
from jax.experimental import pallas as pl
from jax.experimental.pallas import tpu as pltpu
from jax.sharding import PartitionSpec as P


HALVES = 4
GROUPS = (1024, 1024, 1024, 1024, 1024, 1024, 1024)
TAIL = (512, 384, 128)
BM = 256


def _at_end(side):
    col_pos = lax.axis_index("col")
    return jnp.logical_or(col_pos == 0, col_pos == side - 1)


def _mm_kernel(side, own, near, p2, p3, p4, p5, b_ref, *rest):
    out_ref = rest[-1]
    at_end = _at_end(side)
    third = jnp.where(at_end, p3[...], p4[...])
    fourth = jnp.where(at_end, p5[...], p2[...])
    lhs = jnp.concatenate([own[...], near[...], third, fourth], axis=1)
    out_ref[...] = jnp.dot(lhs, b_ref[...], preferred_element_type=jnp.float32).astype(out_ref.dtype)


def _early_kernel(side, own, near, p2, p3, p4, b_ref, out_ref):
    at_end = _at_end(side)
    third = jnp.where(at_end, p3[...], p4[...])
    fourth = jnp.where(at_end, jnp.zeros_like(p2), p2[...])
    lhs = jnp.concatenate([own[...], near[...], third, fourth], axis=1)
    out_ref[...] = jnp.dot(lhs, b_ref[...], preferred_element_type=jnp.float32)


def _late_kernel(side, p5, b_ref, early, c_in, out_ref):
    depth = p5.shape[1]
    fourth = jnp.where(_at_end(side), p5[...], jnp.zeros_like(p5))
    total = early[...] + jnp.dot(fourth, b_ref[-depth:, :], preferred_element_type=jnp.float32)
    out_ref[...] = total.astype(out_ref.dtype)


def _rows(bm, depth, off):
    return pl.BlockSpec((bm, depth), lambda i: (off // bm + i, 0))


def _kept(shape):
    return pl.BlockSpec(shape, lambda i: (0, 0), pipeline_mode=pl.Buffered(1))


def _params(vmem_mib):
    return pltpu.CompilerParams(dimension_semantics=("arbitrary",), vmem_limit_bytes=vmem_mib * 2**20)


def _cost(size, depth, cols):
    return pl.CostEstimate(
        flops=2 * size * depth * cols, bytes_accessed=2 * size * (depth + cols), transcendentals=0
    )


def _group_product(side, own, near, p2, p3, p4, p5, b, c, rows, off, size):
    depth = own.shape[1]
    total, cols = b.shape
    chunk = _rows(BM, depth, off % p2.shape[0])
    piece = _rows(BM, depth, 0)
    full = _rows(BM, depth, off)
    in_specs = [full, full, chunk, chunk, piece, piece, _kept(b.shape)]
    args = [own, near, p2, p3, p4, p5, b]
    alias = {}
    if c is not None:
        in_specs.append(pl.BlockSpec(memory_space=pl.ANY))
        args.append(c)
        alias = {7: 0}
    return pl.pallas_call(
        functools.partial(_mm_kernel, side),
        grid=(size // BM,),
        out_shape=jax.ShapeDtypeStruct((rows, cols), jnp.bfloat16),
        in_specs=in_specs,
        out_specs=_rows(BM, cols, off),
        input_output_aliases=alias,
        compiler_params=_params(8),
        cost_estimate=_cost(size, total, cols),
        name="group_product",
    )(*args)


def _early_product(side, own, near, p2, p3, p4, b, off, size):
    depth = own.shape[1]
    total, cols = b.shape
    bm = BM if size % BM == 0 else BM // 2
    full = _rows(bm, depth, off)
    chunk = _rows(bm, depth, off % p3.shape[0])
    piece = _rows(bm, depth, 0)
    return pl.pallas_call(
        functools.partial(_early_kernel, side),
        grid=(size // bm,),
        out_shape=pltpu.VMEM((size, cols), jnp.float32),
        in_specs=[full, full, chunk, chunk, piece, _kept(b.shape)],
        out_specs=_rows(bm, cols, 0),
        compiler_params=_params(8),
        cost_estimate=_cost(size, total, cols),
        name="early_product",
    )(own, near, p2, p3, p4, b)


def _late_product(side, p5, b, early, c, off, size):
    depth = p5.shape[1]
    rows, cols = c.shape
    bm = BM if size % BM == 0 else BM // 2
    return pl.pallas_call(
        functools.partial(_late_kernel, side),
        grid=(size // bm,),
        out_shape=jax.ShapeDtypeStruct((rows, cols), jnp.bfloat16),
        in_specs=[
            _rows(bm, depth, 0), _kept(b.shape), _rows(bm, cols, 0), pl.BlockSpec(memory_space=pl.ANY),
        ],
        out_specs=_rows(bm, cols, off),
        input_output_aliases={3: 0},
        compiler_params=_params(8),
        cost_estimate=_cost(size, depth, cols),
        name="late_product",
    )(p5, b, early, c)


def _stack_kernel(place_ref, *refs):
    sems = refs[-1]
    out_ref = refs[-2]
    depth = refs[0].shape[0]
    copies = [
        pltpu.make_async_copy(ref, out_ref.at[pl.ds(pl.multiple_of(place_ref[s] * depth, depth), depth)], sems.at[s])
        for s, ref in enumerate(refs[:-2])
    ]
    for copy in copies:
        copy.start()
    for copy in copies:
        copy.wait()


def _stack_blocks(places, blocks):
    count = len(blocks)
    depth, cols = blocks[0].shape
    return pl.pallas_call(
        _stack_kernel,
        out_shape=pltpu.VMEM((count * depth, cols), blocks[0].dtype),
        in_specs=[pl.BlockSpec(memory_space=pltpu.SMEM)] + [pl.BlockSpec(memory_space=pl.ANY)] * count,
        out_specs=pl.BlockSpec(memory_space=pltpu.VMEM),
        scratch_shapes=[pltpu.SemaphoreType.DMA((count,))],
        cost_estimate=pl.CostEstimate(flops=2**20, bytes_accessed=2 * count * depth * cols * 2, transcendentals=0),
        compiler_params=pltpu.CompilerParams(vmem_limit_bytes=12 * 2**20),
        name="stack_blocks",
    )(places, *blocks)


def solution(mesh):
    side = mesh.shape["row"]
    with_near = [(p, p ^ 1) for p in range(side)]
    inner = [(p, side - 1 - p if 0 < p < side - 1 else p) for p in range(side)]

    def local(a, b_own):
        rows, _ = a.shape
        sizes = GROUPS + TAIL
        offs = [sum(sizes[:g]) for g in range(len(sizes))]
        row_pos, col_pos = lax.axis_index("row"), lax.axis_index("col")

        near = lax.ppermute(a, "col", with_near)
        step = rows // HALVES
        p2 = [lax.ppermute(a[h * step : (h + 1) * step], "col", inner) for h in range(HALVES)]
        p3 = [lax.ppermute(x, "col", with_near) for x in p2]
        p4 = [lax.ppermute(near[o : o + s], "col", inner) for o, s in zip(offs, sizes)]
        p5 = [lax.ppermute(x, "col", with_near) for x in p4]

        blocks = [b_own] + [
            lax.ppermute(b_own, "row", [(p, (p - s) % side) for p in range(side)]) for s in range(1, side)
        ]
        b = _stack_blocks(jnp.stack([lax.rem(row_pos + s, side) ^ col_pos for s in range(side)]), blocks)

        main = len(GROUPS)
        early = {}
        for g in range(main, len(sizes)):
            h = offs[g] // step
            early[g] = _early_product(side, a, near, p2[h], p3[h], p4[g], b, offs[g], sizes[g])

        c = None
        for g, (off, size) in enumerate(zip(offs, sizes)):
            h = off // step
            if g < main:
                c = _group_product(side, a, near, p2[h], p3[h], p4[g], p5[g], b, c, rows, off, size)
            else:
                c = _late_product(side, p5[g], b, early[g], c, off, size)
        return c

    return jax.shard_map(
        local, mesh=mesh, in_specs=(P(("dp", "row"), "col"), P("row", "col")),
        out_specs=P(("dp", "row"), "col"), check_vma=False,
    )
```
